512 devices in a mesh: tm: 256 (over z, y, x), chan: 2 (over core).
Axes of the slice: x: 4, y: 8, z: 8, core: 2. Of those that a mesh axis runs over, the one named last changes fastest.
Arguments:
- signal: bfloat16 [3, 32768, 512], P(None, 'tm', 'chan'), may hold values from -6 to 6
- taps: float32 [10, 2, 512], P(None, None, 'chan'), may hold values from -3 to 3
- w_gate: bfloat16 [10, 512, 2, 512], P(None, None, None, 'chan'), may hold values from -0.25 to 0.25
- w_res: bfloat16 [10, 512, 512], P(None, None, 'chan'), may hold values from -0.25 to 0.25
- w_skip: bfloat16 [10, 512, 512], P(None, None, 'chan'), may hold values from -0.1875 to 0.1875
Outputs:
- stream: bfloat16 [3, 32768, 512], P(None, 'tm', 'chan')
- skips: bfloat16 [3, 32768, 512], P(None, 'tm', 'chan')
The draws below stay inside these ranges and needn't reach their ends.
All inputs are finite; a program needn't handle non-finite values.
Results may differ from the reference program's by a relative error of at most 0.02.
Values may be sent and summed in bfloat16 or wider, within the bound.
No kernel may reach another device: no remote copies, remote signals or barrier semaphores. Data moves between devices by JAX's collectives and lax.ppermute only.
A program may use at most 64 MiB of HBM per device.

```python
import jax
import jax.numpy as jnp

C = 512
LAYERS = 10
SEQS = 3
LEN = 32768


def level_of(rng, extent, pieces, low, high):
    gain, own = 1.0, jax.random.fold_in(rng, 6)
    for dim, parts in pieces:
        draws = jnp.exp(jax.random.uniform(jax.random.fold_in(own, dim), (parts,), jnp.float32, low / len(pieces), high / len(pieces)))
        gain = gain * jnp.repeat(draws, extent[dim] // parts).reshape([-1 if axis == dim else 1 for axis in range(len(extent))])
    return gain


def noise(rng, dims, deviation, most, pieces=(), held_as=jnp.bfloat16):
    drawn = jax.random.normal(rng, dims, jnp.float32) * deviation
    if len(pieces) > 0:
        drawn = level_of(rng, dims, pieces, -0.22, 0.18) * drawn
    return jnp.clip(drawn, min=-most, max=most).astype(held_as)


def setup_inputs(seed: int = 0) -> dict:
    streams_of = jax.random.split(jax.random.key(seed), 6)
    signal = noise(streams_of[0], (SEQS, LEN, C), 1.0, 6.0, ((1, 256), (2, 2)))
    taps = noise(streams_of[1], (LAYERS, 2, C), 0.8, 3.0, ((2, 2),), jnp.float32)
    w_gate = noise(streams_of[2], (LAYERS, C, 2, C), C ** -0.5, 0.25, ((3, 2),))
    w_res = noise(streams_of[3], (LAYERS, C, C), C ** -0.5, 0.25, ((2, 2),))
    w_skip = noise(streams_of[4], (LAYERS, C, C), (C * 2) ** -0.5, 0.1875, ((2, 2),))
    return {"signal": signal, "taps": taps, "w_gate": w_gate, "w_res": w_res, "w_skip": w_skip}


def reference(signal, taps, w_gate, w_res, w_skip):
    stream = signal
    skip = jnp.zeros((SEQS, LEN, C), jnp.float32)
    for layer in range(LAYERS):
        delay = 2 ** layer
        delayed = jnp.concatenate([jnp.zeros((SEQS, delay, C), jnp.bfloat16), stream[:, :LEN - delay]], axis=1)
        conv = (taps[layer, 0] * delayed.astype(jnp.float32) + taps[layer, 1] * stream.astype(jnp.float32)).astype(jnp.bfloat16)
        hidden = jnp.einsum("stc,cko->stko", conv.astype(jnp.float32), w_gate[layer].astype(jnp.float32))
        gated = (jnp.tanh(hidden[:, :, 0]) * jax.nn.sigmoid(hidden[:, :, 1])).astype(jnp.bfloat16)
        gated_f = gated.astype(jnp.float32)
        stream = (stream.astype(jnp.float32) + jnp.einsum("stc,co->sto", gated_f, w_res[layer].astype(jnp.float32))).astype(jnp.bfloat16)
        skip = skip + jnp.einsum("stc,co->sto", gated_f, w_skip[layer].astype(jnp.float32))
    return stream, skip.astype(jnp.bfloat16)
```

```python
import functools

import jax
import jax.numpy as jnp
from jax import lax
from jax.experimental import pallas as pl
from jax.experimental.pallas import tpu as pltpu
from jax.sharding import PartitionSpec as P


LOCAL_LAYERS = 7
PAD = 16
BF = jnp.bfloat16
F32 = jnp.float32


def from_earlier(value, steps):
    count = lax.axis_size("tm")
    return lax.ppermute(value, "tm", [(i, i + steps) for i in range(count - steps)])


def other_core(value):
    return lax.ppermute(value, "chan", [(0, 1), (1, 0)])


def dot(a, b):
    return jnp.dot(a, b, preferred_element_type=F32)


def weight_copies(core, pairs, buffers, sems, layers):
    copies = []
    for slot, layer in enumerate(layers):
        row = []
        for which, ((own, other), buf) in enumerate(zip(pairs, buffers)):
            row.append(pltpu.make_async_copy(own.at[layer], buf.at[slot, core], sems.at[slot, 2 * which]))
            row.append(pltpu.make_async_copy(other.at[layer], buf.at[slot, 1 - core], sems.at[slot, 2 * which + 1]))
        copies.append(row)
    return copies


def gated_units(y_ref, z_ref, rows, wg):
    y = y_ref[0:rows]
    for half in range(2):
        f = dot(y, wg[half, 0])
        g = dot(y, wg[half, 1])
        z_ref[0:rows, half * 256 : half * 256 + 256] = (jnp.tanh(f) * (0.5 + 0.5 * jnp.tanh(0.5 * g))).astype(BF)


def first_kernel(halo, own, taps, g_own, g_oth, r_own, r_oth, x_out, z_out, xs, y, z, wg, wr, sems):
    core = lax.axis_index("chan")
    copies = weight_copies(core, ((g_own, g_oth), (r_own, r_oth)), (wg, wr), sems, range(LOCAL_LAYERS))
    for row in copies:
        for copy in row:
            copy.start()
    a0, b0 = PAD, PAD + 256 + PAD
    xs[0:PAD] = jnp.zeros((PAD, 512), F32)
    xs[a0 + 256 : b0] = jnp.zeros((PAD, 512), F32)
    xs[a0 : a0 + 128] = halo[core].astype(F32)
    xs[a0 + 128 : a0 + 256] = own[core].astype(F32)

    @pl.when(core == 0)
    def _():
        xs[b0 : b0 + 128] = halo[2].astype(F32)
        xs[b0 + 128 : b0 + 192] = own[2, 0:64].astype(F32)

    @pl.when(core == 1)
    def _():
        xs[b0 : b0 + 64] = halo[2, 64:128].astype(F32)
        xs[b0 + 64 : b0 + 192] = own[2].astype(F32)

    for layer, first in enumerate((0, 0, 0, 16, 32, 64, 128)):
        delay = 2**layer
        na, nb = 256 - first, 192 - first
        t0, t1 = taps[layer, 0:1], taps[layer, 1:2]
        for base, n, at in ((a0, na, 0), (b0, nb, na)):
            s = base + first
            y[at : at + n] = (t0 * xs[s - delay : s - delay + n] + t1 * xs[s : s + n]).astype(BF)
        rows = na + nb
        for copy in copies[layer]:
            copy.wait()
        gated_units(y, z, rows, wg.at[layer])
        z_out[layer, 0:128] = z[na - 128 : na]
        z_out[layer, 128:192] = z[rows - 64 : rows]
        zv = z[0:rows]
        for half in range(2):
            u = dot(zv, wr[layer, half])
            cols = slice(half * 256, half * 256 + 256)
            for base, n, at in ((a0, na, 0), (b0, nb, na)):
                s = base + first
                new = (xs[s : s + n, cols] + u[at : at + n]).astype(BF)
                if layer < LOCAL_LAYERS - 1:
                    xs[s : s + n, cols] = new.astype(F32)
                elif base == a0:
                    x_out[0:128, cols] = new
                else:
                    x_out[128:192, cols] = new


def second_kernel(x0, x1, x2, x3, taps, g_own, g_oth, r_own, r_oth, x_out, z_out, y, z, xs, wg, wr, sems):
    core = lax.axis_index("chan")
    copies = weight_copies(core, ((g_own, g_oth), (r_own, r_oth)), (wg, wr), sems, (7, 8))
    for row in copies:
        for copy in row:
            copy.start()
    t0, t1 = taps[7, 0:1], taps[7, 1:2]
    y[0:192] = (t0 * x1[...].astype(F32) + t1 * x0[...].astype(F32)).astype(BF)
    y[192:384] = (t0 * x3[...].astype(F32) + t1 * x2[...].astype(F32)).astype(BF)
    for copy in copies[0]:
        copy.wait()
    gated_units(y, z, 384, wg.at[0])
    z_out[0] = z[0:192]
    zv = z[0:384]
    for half in range(2):
        cols = slice(half * 256, half * 256 + 256)
        u = dot(zv, wr[0, half])
        xs[0:192, cols] = (x0[:, cols].astype(F32) + u[0:192]).astype(BF)
        xs[192:384, cols] = (x2[:, cols].astype(F32) + u[192:384]).astype(BF)
    t0, t1 = taps[8, 0:1], taps[8, 1:2]
    y[0:192] = (t0 * xs[192:384].astype(F32) + t1 * xs[0:192].astype(F32)).astype(BF)
    for copy in copies[1]:
        copy.wait()
    gated_units(y, z, 192, wg.at[1])
    z_out[1] = z[0:192]
    zv = z[0:192]
    for half in range(2):
        cols = slice(half * 256, half * 256 + 256)
        u = dot(zv, wr[1, half])
        x_out[:, cols] = (xs[0:192, cols].astype(F32) + u).astype(BF)


def third_kernel(x0, x4, skip, taps, g_own, g_oth, r_own, r_oth, s_own, s_oth, out, y, z, wg, wr, ws, sems):
    core = lax.axis_index("chan")
    copies = weight_copies(core, ((g_own, g_oth), (r_own, r_oth), (s_own, s_oth)), (wg, wr, ws), sems, (9,))
    for copy in copies[0]:
        copy.start()
    t0, t1 = taps[9, 0:1], taps[9, 1:2]
    y[...] = (t0 * x4[...].astype(F32) + t1 * x0[...].astype(F32)).astype(BF)
    for copy in copies[0]:
        copy.wait()
    gated_units(y, z, 192, wg.at[0])
    zv = z[...]
    for half in range(2):
        cols = slice(half * 256, half * 256 + 256)
        out[0:192, cols] = (x0[:, cols].astype(F32) + dot(zv, wr[0, half])).astype(BF)
        out[192:384, cols] = (skip[:, cols] + dot(zv, ws[0, half])).astype(BF)


def skip_kernel(first, layers, z, before, s_own, s_oth, out, ws, sems):
    core = lax.axis_index("chan")
    copies = weight_copies(core, ((s_own, s_oth),), (ws,), sems, range(first, first + layers))
    for row in copies:
        for copy in row:
            copy.start()
    for layer in range(layers):
        for copy in copies[layer]:
            copy.wait()
    for half in range(2):
        cols = slice(half * 256, half * 256 + 256)
        total = dot(z[0], ws[0, half])
        for layer in range(1, layers):
            total = total + dot(z[layer], ws[layer, half])
        if before is not None:
            total = total + before[:, cols]
        out[:, cols] = total


def skip_first(first, layers, z, s_own, s_oth, out, ws, sems):
    skip_kernel(first, layers, z, None, s_own, s_oth, out, ws, sems)


def last_kernel(g, stream, skips):
    core = lax.axis_index("chan")
    for half in range(2):

        @pl.when(core == half)
        def _():
            cols = slice(half * 256, half * 256 + 256)
            for out, at in ((stream, 0), (skips, 192)):
                for k in range(2):
                    out[k] = g[k, at : at + 128, cols]
                    out[2, k * 64 : k * 64 + 64] = g[k, at + 128 : at + 192, cols]


def spec():
    return pl.BlockSpec(memory_space=pltpu.VMEM)


def anywhere():
    return pl.BlockSpec(memory_space=pl.ANY)


def call(body, inputs, outs, in_specs, scratch, flops, name):
    moved = sum(v.size * v.dtype.itemsize for v in inputs)
    return pl.pallas_call(
        body,
        out_shape=outs,
        in_specs=in_specs,
        out_specs=jax.tree.map(lambda _: spec(), outs),
        scratch_shapes=scratch,
        cost_estimate=pl.CostEstimate(flops=flops, bytes_accessed=moved, transcendentals=0),
        compiler_params=pltpu.CompilerParams(vmem_limit_bytes=40 * 2**20),
        name=name,
    )(*inputs)


def local(signal, taps, w_gate, w_res, w_skip):
    halo = from_earlier(signal, 1)
    r_oth = other_core(w_res)
    g_own = jnp.transpose(w_gate, (0, 2, 1, 3))
    g_oth = other_core(g_own)
    s_oth = other_core(w_skip)
    own = lax.all_gather(signal, "chan", axis=2, tiled=True)
    taps = lax.all_gather(taps, "chan", axis=2, tiled=True)
    halo = lax.all_gather(halo, "chan", axis=2, tiled=True)
    weights = [g_own, g_oth, w_res, r_oth]
    sds = jax.ShapeDtypeStruct
    vm = pltpu.VMEM
    x7, z_a = call(
        first_kernel,
        [halo, own, taps, *weights],
        (sds((192, 512), BF), sds((LOCAL_LAYERS, 192, 512), BF)),
        [spec()] * 3 + [anywhere()] * 4,
        [
            vm((3 * PAD + 448, 512), F32),
            vm((448, 512), BF),
            vm((448, 512), BF),
            vm((LOCAL_LAYERS, 2, 2, 512, 256), BF),
            vm((LOCAL_LAYERS, 2, 512, 256), BF),
            pltpu.SemaphoreType.DMA((LOCAL_LAYERS, 4)),
        ],
        7 * 400 * 512 * 1536 * 2,
        "layers_0_6",
    )
    x7s = [from_earlier(x7, d) for d in (1, 2, 3)]
    skip = call(
        functools.partial(skip_first, 0, LOCAL_LAYERS),
        [z_a, w_skip, s_oth],
        sds((192, 512), F32),
        [spec()] + [anywhere()] * 2,
        [vm((LOCAL_LAYERS, 2, 512, 256), BF), pltpu.SemaphoreType.DMA((LOCAL_LAYERS, 2))],
        LOCAL_LAYERS * 192 * 512 * 512 * 2,
        "skip_0_6",
    )
    x9, z_b = call(
        second_kernel,
        [x7, *x7s, taps, *weights],
        (sds((192, 512), BF), sds((2, 192, 512), BF)),
        [spec()] * 5 + [anywhere()] * 4,
        [
            vm((384, 512), BF),
            vm((384, 512), BF),
            vm((384, 512), BF),
            vm((2, 2, 2, 512, 256), BF),
            vm((2, 2, 512, 256), BF),
            pltpu.SemaphoreType.DMA((2, 4)),
        ],
        3 * 192 * 512 * 1536 * 2,
        "layers_7_8",
    )
    x9_far = from_earlier(x9, 4)
    skip = call(
        functools.partial(skip_kernel, 7, 2),
        [z_b, skip, w_skip, s_oth],
        sds((192, 512), F32),
        [spec()] * 2 + [anywhere()] * 2,
        [vm((2, 2, 512, 256), BF), pltpu.SemaphoreType.DMA((2, 2))],
        2 * 192 * 512 * 512 * 2,
        "skip_7_8",
    )
    both = call(
        third_kernel,
        [x9, x9_far, skip, taps, *weights, w_skip, s_oth],
        sds((384, 512), BF),
        [spec()] * 4 + [anywhere()] * 6,
        [
            vm((192, 512), BF),
            vm((192, 512), BF),
            vm((1, 2, 2, 512, 256), BF),
            vm((1, 2, 512, 256), BF),
            vm((1, 2, 512, 256), BF),
            pltpu.SemaphoreType.DMA((1, 6)),
        ],
        192 * 512 * 2048 * 2,
        "layer_9",
    )
    both = lax.all_gather(both, "chan", axis=0)
    return call(
        last_kernel,
        [both],
        (sds((3, 128, 256), BF), sds((3, 128, 256), BF)),
        [spec()],
        [],
        1,
        "outputs",
    )


def solution(mesh):
    in_specs = (
        P(None, "tm", "chan"),
        P(None, None, "chan"),
        P(None, None, None, "chan"),
        P(None, None, "chan"),
        P(None, None, "chan"),
    )
    out_specs = (P(None, "tm", "chan"), P(None, "tm", "chan"))
    return jax.shard_map(local, mesh=mesh, in_specs=in_specs, out_specs=out_specs, check_vma=False)
```

```python
import jax
import jax.numpy as jnp
from jax import lax
from jax.experimental import pallas as pl
from jax.experimental.pallas import tpu as pltpu
from jax.sharding import PartitionSpec as P


PAD = 16
A0 = PAD
A_FIRST = (0, 0, 0, 16, 32, 64, 128)
B_FIRST = (0, 0, 0, 0, 16, 32, 64)
HALVES = (slice(0, 256), slice(256, 512))
BF = jnp.bfloat16
F32 = jnp.float32


def from_earlier(value, steps):
    count = lax.axis_size("tm")
    return lax.ppermute(value, "tm", [(i, i + steps) for i in range(count - steps)])


def from_two(value, steps):
    count = lax.axis_size("tm")
    pairs = [(2 * i + c, 2 * (i + steps[c]) + c) for c in range(2) for i in range(count - steps[c])]
    return lax.ppermute(value, ("tm", "chan"), pairs)


def other_core(value):
    return lax.ppermute(value, "chan", [(0, 1), (1, 0)])


def dot(a, b):
    return jnp.dot(a, b, preferred_element_type=F32)


def columns():
    core = lax.axis_index("chan")
    own = pl.ds(pl.multiple_of(core * 256, 256), 256)
    other = pl.ds(pl.multiple_of((1 - core) * 256, 256), 256)
    return core, own, other


def rows_own_first(w, order):
    return jnp.concatenate([w[rows] for rows in order], axis=0)


def gated_units(y_ref, z_ref, rows, weights, order):
    y = y_ref[0:rows]
    for w, cols in zip(weights, HALVES):
        f = dot(y, rows_own_first(w.at[0], order))
        g = dot(y, rows_own_first(w.at[1], order))
        z_ref[0:rows, cols] = (jnp.tanh(f) * (0.5 + 0.5 * jnp.tanh(0.5 * g))).astype(BF)


def first_kernel(own, h1, h2, t_own, t_oth, g_own, g_oth, r_own, r_oth, x_out, z_out, taps, xa, xb, xp, y, z):
    core, *order = columns()
    for part, cols in zip((t_own, t_oth), HALVES):
        taps[:, :, cols] = part[...]
    zero = jnp.zeros((PAD, 512), F32)
    xa[0:PAD] = zero
    xb[:, 0:PAD] = jnp.zeros((4, PAD, 128), F32)
    xp[0:PAD] = zero
    blocks = ((h2, 1), (h1, 1), (h2, 0), (h1, 0))

    def load(rows, source):
        for given, cols in zip(order, HALVES):
            xa[rows, cols] = source[core, :, given].astype(F32)
            shared = source[2, :, given].astype(F32)
            for j in range(2):
                xb[cols.start // 128 + j, rows] = shared[:, 128 * j : 128 * j + 128]

    for k, (h, i) in enumerate(blocks):
        load(slice(A0 + 128 * k, A0 + 128 * k + 128), h.at[i])
    load(slice(A0 + 512, A0 + 640), own)

    for layer in range(7):
        delay = 2**layer
        first, first_b = A_FIRST[layer], B_FIRST[layer]
        na, nb = 640 - first, 320 - first_b
        rows = na + nb
        t0, t1 = taps[layer, 0:1], taps[layer, 1:2]
        s = A0 + first
        y[0:na] = (t0 * xa[s - delay : s - delay + na] + t1 * xa[s : s + na]).astype(BF)
        if layer == 0:
            for c in range(2):

                @pl.when(core == c)
                def _(c=c):
                    for j in range(4):
                        lanes = slice(128 * j, 128 * j + 128)
                        now = xb[j, pl.ds(PAD + c, 320, stride=2)]
                        before = xb[j, pl.ds(PAD + c - 1, 320, stride=2)]
                        y[640:960, lanes] = (t0[:, lanes] * before + t1[:, lanes] * now).astype(BF)
                        xp[PAD : PAD + 320, lanes] = now

        else:
            s = PAD + first_b
            half = delay // 2
            y[na:rows] = (t0 * xp[s - half : s - half + nb] + t1 * xp[s : s + nb]).astype(BF)
        gated_units(y, z, rows, (g_own.at[layer], g_oth.at[layer]), order)
        z_out[layer, 0:128] = z[na - 128 : na]
        z_out[layer, 128:192] = z[rows - 64 : rows]
        zv = z[0:rows]
        for w, cols in zip((r_own, r_oth), HALVES):
            u = dot(zv, rows_own_first(w.at[layer], order))
            for ref, s, n, at in ((xa, A0 + first, na, 0), (xp, PAD + first_b, nb, na)):
                ref[s : s + n, cols] = (ref[s : s + n, cols] + u[at : at + n]).astype(BF).astype(F32)

    def block(k):
        a, b = A0 + 512 - 128 * k, PAD + 256 - 64 * k
        return ((xa, slice(a, a + 128)), (xp, slice(b, b + 64)))

    for layer, targets, far in ((7, (0, 2), 1), (8, (0,), 2)):
        t0, t1 = taps[layer, 0:1], taps[layer, 1:2]
        at = 0
        for k in targets:
            for (ref, now), (_, before) in zip(block(k), block(k + far)):
                n = now.stop - now.start
                y[at : at + n] = (t0 * ref[before] + t1 * ref[now]).astype(BF)
                at += n
        rows = at
        gated_units(y, z, rows, (g_own.at[layer], g_oth.at[layer]), order)
        z_out[layer] = z[0:192]
        zv = z[0:rows]
        for w, cols in zip((r_own, r_oth), HALVES):
            u = dot(zv, rows_own_first(w.at[layer], order))
            at = 0
            for k in targets:
                for ref, now in block(k):
                    n = now.stop - now.start
                    new = (ref[now, cols] + u[at : at + n]).astype(BF)
                    if layer == 8:
                        x_out[at : at + n, cols] = new
                    else:
                        ref[now, cols] = new.astype(F32)
                    at += n


def last_layer(x0, x4, skip, taps, g_own, g_oth, r_own, r_oth, s_own, s_oth, out, y, z):
    _, *order = columns()
    t0, t1 = taps[9, 0:1], taps[9, 1:2]
    y[...] = (t0 * x4[...].astype(F32) + t1 * x0[...].astype(F32)).astype(BF)
    gated_units(y, z, 192, (g_own.at[9], g_oth.at[9]), order)
    zv = z[...]
    for r, s, cols in zip((r_own, r_oth), (s_own, s_oth), HALVES):
        out[0:192, cols] = (x0[:, cols].astype(F32) + dot(zv, rows_own_first(r.at[9], order))).astype(BF)
        out[192:384, cols] = (skip[:, cols] + dot(zv, rows_own_first(s.at[9], order))).astype(BF)


def skip_kernel(z, s_own, s_oth, out):
    _, *order = columns()
    for s, cols in zip((s_own, s_oth), HALVES):
        total = dot(z[0], rows_own_first(s.at[0], order))
        for layer in range(1, 9):
            total = total + dot(z[layer], rows_own_first(s.at[layer], order))
        out[:, cols] = total


def outputs_kernel(g, stream, skips, mixed):
    core = lax.axis_index("chan")
    for half in range(2):

        @pl.when(core == half)
        def _(half=half):
            for out, at in ((stream, 0), (skips, 192)):
                for k in range(2):
                    cols = HALVES[0 if k == half else 1]
                    out[k] = g[k, at : at + 128, cols]
                    for j in range(2):
                        lanes = slice(cols.start + 128 * j, cols.start + 128 * j + 128)
                        mixed[j, pl.ds(k, 64, stride=2)] = g[k, at + 128 : at + 192, lanes].astype(F32)
                for j in range(2):
                    out[2, :, 128 * j : 128 * j + 128] = mixed[j].astype(BF)


def call(body, inputs, outs, scratch, flops, space=pltpu.VMEM):
    moved = sum(v.size * v.dtype.itemsize for v in inputs)
    vmem = pl.BlockSpec(memory_space=pltpu.VMEM)
    return pl.pallas_call(
        body,
        out_shape=outs,
        in_specs=[pl.BlockSpec(memory_space=space)] * len(inputs),
        out_specs=jax.tree.map(lambda _: vmem, outs),
        scratch_shapes=scratch,
        cost_estimate=pl.CostEstimate(flops=flops, bytes_accessed=moved, transcendentals=0),
        compiler_params=pltpu.CompilerParams(vmem_limit_bytes=24 * 2**20),
    )(*inputs)


def relayout_kernel(w, out, raw, sems):
    copies = [pltpu.make_async_copy(w.at[layer], raw.at[layer], sems.at[layer]) for layer in range(10)]
    for copy in copies:
        copy.start()
    for layer in range(10):
        copies[layer].wait()
        both = raw[layer].reshape(512, 512)
        out[layer, 0] = both[:, :256]
        out[layer, 1] = both[:, 256:]


def local(signal, taps, w_gate, w_res, w_skip):
    sds = jax.ShapeDtypeStruct
    vm = pltpu.VMEM
    own = lax.all_gather(signal, "chan", axis=2, tiled=True)
    h1 = from_two(own, (1, 3))
    h2 = from_two(own, (2, 4))
    r_oth = other_core(w_res)
    g_own = call(
        relayout_kernel,
        [w_gate],
        sds((10, 2, 512, 256), BF),
        [vm((10, 512, 2, 256), BF), pltpu.SemaphoreType.DMA((10,))],
        10**7,
        pltpu.HBM,
    )
    g_oth = other_core(g_own)
    t_oth = other_core(taps)
    s_oth = other_core(w_skip)
    h1 = lax.all_gather(h1, "chan", axis=0)
    h2 = lax.all_gather(h2, "chan", axis=0)
    weights = [g_own, g_oth, w_res, r_oth]
    x9, zs, taps_all = call(
        first_kernel,
        [own, h1, h2, taps, t_oth, *weights],
        (sds((192, 512), BF), sds((9, 192, 512), BF), sds((10, 2, 512), F32)),
        [
            vm((PAD + 640, 512), F32),
            vm((4, PAD + 640, 128), F32),
            vm((PAD + 320, 512), F32),
            vm((960, 512), BF),
            vm((960, 512), BF),
        ],
        7000 * 512 * 1536 * 2,
    )
    x9_far = from_earlier(x9, 4)
    skip = call(skip_kernel, [zs, w_skip, s_oth], sds((192, 512), F32), [], 9 * 192 * 512 * 512 * 2)
    both = call(
        last_layer,
        [x9, x9_far, skip, taps_all, *weights, w_skip, s_oth],
        sds((384, 512), BF),
        [vm((192, 512), BF), vm((192, 512), BF)],
        192 * 512 * 2048 * 2,
    )
    both = lax.all_gather(both, "chan", axis=0)
    return call(outputs_kernel, [both], (sds((3, 128, 256), BF), sds((3, 128, 256), BF)), [vm((2, 128, 128), F32)], 1)


def solution(mesh):
    in_specs = (
        P(None, "tm", "chan"),
        P(None, None, "chan"),
        P(None, None, None, "chan"),
        P(None, None, "chan"),
        P(None, None, "chan"),
    )
    out_specs = (P(None, "tm", "chan"), P(None, "tm", "chan"))
    return jax.shard_map(local, mesh=mesh, in_specs=in_specs, out_specs=out_specs, check_vma=False)
```

```python
import functools

import jax
import jax.numpy as jnp
from jax import lax
from jax.experimental import pallas as pl
from jax.experimental.pallas import tpu as pltpu
from jax.sharding import PartitionSpec as P


PAD = 16
MIB_A, MIB_B = 47, 24
SPLIT = 6
A0 = PAD
A_FIRST = (0, 0, 0, 16, 32, 64, 128)
B_FIRST = (0, 0, 0, 0, 16, 32, 64)
HALVES = (slice(0, 256), slice(256, 512))
BF = jnp.bfloat16
F32 = jnp.float32


def from_earlier(value, steps):
    count = lax.axis_size("tm")
    return lax.ppermute(value, "tm", [(i, i + steps) for i in range(count - steps)])


def from_two(value, steps):
    count = lax.axis_size("tm")
    pairs = [(2 * i + c, 2 * (i + steps[c]) + c) for c in range(2) for i in range(count - steps[c])]
    return lax.ppermute(value, ("tm", "chan"), pairs)


def other_core(value):
    return lax.ppermute(value, "chan", [(0, 1), (1, 0)])


def dot(a, b):
    return jnp.dot(a, b, preferred_element_type=F32)


def row_order():
    core = lax.axis_index("chan")
    return core, (pl.multiple_of(core * 256, 256), pl.multiple_of(256 - core * 256, 256))


def rows_own_first(w, order, at=0):
    return jnp.concatenate([w[pl.ds(at + start, 256)] for start in order], axis=0)


def gated_units(y_ref, z_ref, rows, weights, at, order):
    y = y_ref[0:rows]
    for w, cols in zip(weights, HALVES):
        f = dot(y, rows_own_first(w, order, at))
        g = dot(y, rows_own_first(w, order, at + 512))
        z_ref[0:rows, cols] = (jnp.tanh(f) * (0.5 + 0.5 * jnp.tanh(0.5 * g))).astype(BF)


def first_kernel(own, h1, h2, t_own, ga_own, ga_oth, gb_own, gb_oth, r_own, r_oth, x_out, z_out, taps, xa, xb, xp, y, z):
    core, order = row_order()
    taps[:, :, HALVES[0]] = t_own[...]
    for tap in range(2):
        at = 1024 * (10 - SPLIT) + 48 * tap
        parts = [gb_oth[at + 16 * part : at + 16 * part + 10].astype(F32) for part in range(3)]
        taps[:, tap, HALVES[1]] = parts[0] + parts[1] + parts[2]

    def gate(layer):
        return ((ga_own, ga_oth), 1024 * layer) if layer < SPLIT else ((gb_own, gb_oth), 1024 * (layer - SPLIT))

    zero = jnp.zeros((PAD, 512), F32)
    xa[0:PAD] = zero
    xb[:, 0:PAD] = jnp.zeros((4, PAD, 128), F32)
    xp[0:PAD] = zero
    blocks = ((h2, 1), (h2, 0), (h1, 1), (h1, 0))

    def load(rows, source):
        for start, cols in zip(order, HALVES):
            given = pl.ds(start, 256)
            xa[rows, cols] = source[core, :, given].astype(F32)
            shared = source[2, :, given].astype(F32)
            for j in range(2):
                xb[cols.start // 128 + j, rows] = shared[:, 128 * j : 128 * j + 128]

    for k, (h, i) in enumerate(blocks):
        load(slice(A0 + 128 * k, A0 + 128 * k + 128), h.at[i])
    load(slice(A0 + 512, A0 + 640), own)

    for layer in range(7):
        delay = 2**layer
        first, first_b = A_FIRST[layer], B_FIRST[layer]
        na, nb = 640 - first, 320 - first_b
        rows = na + nb
        t0, t1 = taps[layer, 0:1], taps[layer, 1:2]
        s = A0 + first
        y[0:na] = (t0 * xa[s - delay : s - delay + na] + t1 * xa[s : s + na]).astype(BF)
        if layer == 0:
            for c in range(2):

                @pl.when(core == c)
                def _(c=c):
                    for j in range(4):
                        lanes = slice(128 * j, 128 * j + 128)
                        now = xb[j, pl.ds(PAD + c, 320, stride=2)]
                        before = xb[j, pl.ds(PAD + c - 1, 320, stride=2)]
                        y[640:960, lanes] = (t0[:, lanes] * before + t1[:, lanes] * now).astype(BF)
                        xp[PAD : PAD + 320, lanes] = now

        else:
            s = PAD + first_b
            half = delay // 2
            y[na:rows] = (t0 * xp[s - half : s - half + nb] + t1 * xp[s : s + nb]).astype(BF)
        gated_units(y, z, rows, *gate(layer), order)
        z_out[layer, 0:128] = z[na - 128 : na]
        z_out[layer, 128:192] = z[rows - 64 : rows]
        zv = z[0:rows]
        for w, cols in zip((r_own, r_oth), HALVES):
            u = dot(zv, rows_own_first(w.at[layer], order))
            for ref, s, n, at in ((xa, A0 + first, na, 0), (xp, PAD + first_b, nb, na)):
                ref[s : s + n, cols] = (ref[s : s + n, cols] + u[at : at + n]).astype(BF).astype(F32)

    def block(k):
        a, b = A0 + 512 - 128 * k, PAD + 256 - 64 * k
        return ((xa, slice(a, a + 128)), (xp, slice(b, b + 64)))

    for layer, targets, far in ((7, (0, 2), 1), (8, (0,), 2)):
        t0, t1 = taps[layer, 0:1], taps[layer, 1:2]
        at = 0
        for k in targets:
            for (ref, now), (_, before) in zip(block(k), block(k + far)):
                n = now.stop - now.start
                y[at : at + n] = (t0 * ref[before] + t1 * ref[now]).astype(BF)
                at += n
        rows = at
        gated_units(y, z, rows, *gate(layer), order)
        z_out[layer] = z[0:192]
        zv = z[0:rows]
        for w, cols in zip((r_own, r_oth), HALVES):
            u = dot(zv, rows_own_first(w.at[layer], order))
            at = 0
            for k in targets:
                for ref, now in block(k):
                    n = now.stop - now.start
                    new = (ref[now, cols] + u[at : at + n]).astype(BF)
                    if layer == 8:
                        x_out[at : at + n, cols] = new
                    else:
                        ref[now, cols] = new.astype(F32)
                    at += n


def last_layer(x0, x4, skip, taps, g_own, g_oth, r_own, r_oth, s_own, s_oth, out, y, z):
    _, order = row_order()
    t0, t1 = taps[9, 0:1], taps[9, 1:2]
    y[...] = (t0 * x4[...].astype(F32) + t1 * x0[...].astype(F32)).astype(BF)
    gated_units(y, z, 192, (g_own, g_oth), 1024 * (9 - SPLIT), order)
    zv = z[...]
    for r, s, cols in zip((r_own, r_oth), (s_own, s_oth), HALVES):
        out[0:192, cols] = (x0[:, cols].astype(F32) + dot(zv, rows_own_first(r.at[9], order))).astype(BF)
        out[192:384, cols] = (skip[:, cols] + dot(zv, rows_own_first(s.at[9], order))).astype(BF)


def skip_kernel(z, s_own, s_oth, out):
    _, order = row_order()
    for s, cols in zip((s_own, s_oth), HALVES):
        total = dot(z[0], rows_own_first(s.at[0], order))
        for layer in range(1, 9):
            total = total + dot(z[layer], rows_own_first(s.at[layer], order))
        out[:, cols] = total


def outputs_kernel(g, stream, skips, mixed):
    core = lax.axis_index("chan")
    for half in range(2):

        @pl.when(core == half)
        def _(half=half):
            for out, at in ((stream, 0), (skips, 192)):
                for k in range(2):
                    cols = HALVES[0 if k == half else 1]
                    out[k] = g[k, at : at + 128, cols]
                    for j in range(2):
                        lanes = slice(cols.start + 128 * j, cols.start + 128 * j + 128)
                        mixed[j, pl.ds(k, 64, stride=2)] = g[k, at + 128 : at + 192, lanes].astype(F32)
                for j in range(2):
                    out[2, :, 128 * j : 128 * j + 128] = mixed[j].astype(BF)


def call(body, inputs, outs, scratch, flops, spaces=None, vmem_mib=24):
    moved = sum(v.size * v.dtype.itemsize for v in inputs)
    vmem = pl.BlockSpec(memory_space=pltpu.VMEM)
    return pl.pallas_call(
        body,
        out_shape=outs,
        in_specs=[pl.BlockSpec(memory_space=one) for one in spaces or [pltpu.VMEM] * len(inputs)],
        out_specs=jax.tree.map(lambda _: vmem, outs),
        scratch_shapes=scratch,
        cost_estimate=pl.CostEstimate(flops=flops, bytes_accessed=moved, transcendentals=0),
        compiler_params=pltpu.CompilerParams(vmem_limit_bytes=vmem_mib * 2**20),
    )(*inputs)


def relayout_kernel(first, count, *refs):
    *taps, w, out, raw, sems = refs
    copies = [pltpu.make_async_copy(w.at[first + i], raw.at[i], sems.at[i]) for i in range(count)]
    for copy in copies:
        copy.start()
    for tap in range(2 if taps else 0):
        rest = taps[0][:, tap]
        for part in range(3):
            value = rest.astype(BF)
            rest = rest - value.astype(F32)
            at = count * 1024 + 48 * tap + 16 * part
            out[at : at + 10] = value
            out[at + 10 : at + 16] = jnp.zeros((6, 256), BF)
    for i, copy in enumerate(copies):
        copy.wait()
        both = raw[i].reshape(512, 512)
        out[1024 * i : 1024 * i + 512] = both[:, :256]
        out[1024 * i + 512 : 1024 * i + 1024] = both[:, 256:]


def relayout(first, count, vmem_mib, w_gate, *taps):
    return call(
        functools.partial(relayout_kernel, first, count),
        [*taps, w_gate],
        jax.ShapeDtypeStruct((count * 1024 + 96 * len(taps), 256), BF),
        [pltpu.VMEM((count, 512, 2, 256), BF), pltpu.SemaphoreType.DMA((count,))],
        10**6,
        [pltpu.VMEM] * len(taps) + [pltpu.HBM],
        vmem_mib,
    )


def local(signal, taps, w_gate, w_res, w_skip):
    sds = jax.ShapeDtypeStruct
    vm = pltpu.VMEM
    own = lax.all_gather(signal, "chan", axis=2, tiled=True)
    h1 = from_two(own, (1, 2))
    h2 = from_two(own, (3, 4))
    r_oth = other_core(w_res)
    ga_own = relayout(0, SPLIT, MIB_A, w_gate)
    ga_oth = other_core(ga_own)
    gb_own = relayout(SPLIT, 10 - SPLIT, MIB_B, w_gate, taps)
    gb_oth = other_core(gb_own)
    s_oth = other_core(w_skip)
    h1 = lax.all_gather(h1, "chan", axis=0)
    h2 = lax.all_gather(h2, "chan", axis=0)
    x9, zs, taps_all = call(
        first_kernel,
        [own, h1, h2, taps, ga_own, ga_oth, gb_own, gb_oth, w_res, r_oth],
        (sds((192, 512), BF), sds((9, 192, 512), BF), sds((10, 2, 512), F32)),
        [
            vm((PAD + 640, 512), F32),
            vm((4, PAD + 640, 128), F32),
            vm((PAD + 320, 512), F32),
            vm((960, 512), BF),
            vm((960, 512), BF),
        ],
        7000 * 512 * 1536 * 2,
    )
    x9_far = from_earlier(x9, 4)
    skip = call(skip_kernel, [zs, w_skip, s_oth], sds((192, 512), F32), [], 9 * 192 * 512 * 512 * 2)
    both = call(
        last_layer,
        [x9, x9_far, skip, taps_all, gb_own, gb_oth, w_res, r_oth, w_skip, s_oth],
        sds((384, 512), BF),
        [vm((192, 512), BF), vm((192, 512), BF)],
        192 * 512 * 2048 * 2,
    )
    both = lax.all_gather(both, "chan", axis=0)
    return call(outputs_kernel, [both], (sds((3, 128, 256), BF), sds((3, 128, 256), BF)), [vm((2, 128, 128), F32)], 1)


def solution(mesh):
    in_specs = (
        P(None, "tm", "chan"),
        P(None, None, "chan"),
        P(None, None, None, "chan"),
        P(None, None, "chan"),
        P(None, None, "chan"),
    )
    out_specs = (P(None, "tm", "chan"), P(None, "tm", "chan"))
    return jax.shard_map(local, mesh=mesh, in_specs=in_specs, out_specs=out_specs, check_vma=False)
```

```python
import functools

import jax
import jax.numpy as jnp
from jax import lax
from jax.experimental import pallas as pl
from jax.experimental.pallas import tpu as pltpu
from jax.sharding import PartitionSpec as P


PAD = 16
MIB_A, MIB_B = 47, 24
SPLIT = 5
A0 = PAD
A_FIRST = (0, 0, 0, 16, 32, 64, 128)
B_FIRST = (0, 0, 0, 0, 16, 32, 64)
HALVES = (slice(0, 256), slice(256, 512))
BF = jnp.bfloat16
F32 = jnp.float32


def from_earlier(value, steps):
    count = lax.axis_size("tm")
    return lax.ppermute(value, "tm", [(i, i + steps) for i in range(count - steps)])


def from_two(value, steps):
    count = lax.axis_size("tm")
    pairs = [(2 * i + c, 2 * (i + steps[c]) + c) for c in range(2) for i in range(count - steps[c])]
    return lax.ppermute(value, ("tm", "chan"), pairs)


def other_core(value):
    return lax.ppermute(value, "chan", [(0, 1), (1, 0)])


def dot(a, b):
    return jnp.dot(a, b, preferred_element_type=F32)


def row_order():
    core = lax.axis_index("chan")
    return core, (pl.multiple_of(core * 256, 256), pl.multiple_of(256 - core * 256, 256))


def rows_own_first(w, order, at=0):
    return jnp.concatenate([w[pl.ds(at + start, 256)] for start in order], axis=0)


def gated_units(y_ref, z_ref, rows, weights, at, order):
    y = y_ref[0:rows]
    for w, cols in zip(weights, HALVES):
        f = dot(y, rows_own_first(w, order, at))
        g = dot(y, rows_own_first(w, order, at + 512))
        z_ref[0:rows, cols] = (jnp.tanh(f) * (0.5 + 0.5 * jnp.tanh(0.5 * g))).astype(BF)


def first_kernel(own, h1, h2, t_own, ga_own, ga_oth, gb_own, gb_oth, r_own, r_oth, x_out, z_out, taps, xa, xb, xp, y, z):
    core, order = row_order()
    taps[:, :, HALVES[0]] = t_own[...]
    for tap in range(2):
        at = 1024 * (10 - SPLIT) + 48 * tap
        parts = [gb_oth[at + 16 * part : at + 16 * part + 10].astype(F32) for part in range(3)]
        taps[:, tap, HALVES[1]] = parts[0] + parts[1] + parts[2]

    def gate(layer):
        return ((ga_own, ga_oth), 1024 * layer) if layer < SPLIT else ((gb_own, gb_oth), 1024 * (layer - SPLIT))

    zero = jnp.zeros((PAD, 512), F32)
    xa[0:PAD] = zero
    xb[:, 0:PAD] = jnp.zeros((4, PAD, 128), F32)
    xp[0:PAD] = zero
    blocks = ((h2, 0), (h2, 1), (h1, 1), (h1, 0))

    def load(rows, source):
        for start, cols in zip(order, HALVES):
            given = pl.ds(start, 256)
            xa[rows, cols] = source[core, :, given].astype(F32)
            shared = source[2, :, given].astype(F32)
            for j in range(2):
                xb[cols.start // 128 + j, rows] = shared[:, 128 * j : 128 * j + 128]

    for k, (h, i) in enumerate(blocks):
        load(slice(A0 + 128 * k, A0 + 128 * k + 128), h.at[i])
    load(slice(A0 + 512, A0 + 640), own)

    for layer in range(7):
        delay = 2**layer
        first, first_b = A_FIRST[layer], B_FIRST[layer]
        na, nb = 640 - first, 320 - first_b
        rows = na + nb
        t0, t1 = taps[layer, 0:1], taps[layer, 1:2]
        s = A0 + first
        y[0:na] = (t0 * xa[s - delay : s - delay + na] + t1 * xa[s : s + na]).astype(BF)
        if layer == 0:
            for j in range(4):
                lanes = slice(128 * j, 128 * j + 128)
                now = xb[j, pl.ds(PAD + core, 320, stride=2)]
                before = xb[j, pl.ds(PAD - 1 + core, 320, stride=2)]
                y[640:960, lanes] = (t0[:, lanes] * before + t1[:, lanes] * now).astype(BF)
                xp[PAD : PAD + 320, lanes] = now
        else:
            s = PAD + first_b
            half = delay // 2
            y[na:rows] = (t0 * xp[s - half : s - half + nb] + t1 * xp[s : s + nb]).astype(BF)
        for lo, hi in ((0, na), (na, rows)):
            gated_units(y.at[lo:hi], z.at[lo:hi], hi - lo, *gate(layer), order)
        z_out[layer, 0:128] = z[na - 128 : na]
        z_out[layer, 128:192] = z[rows - 64 : rows]
        for ref, s, n, at in ((xa, A0 + first, na, 0), (xp, PAD + first_b, nb, na)):
            zv = z[at : at + n]
            for w, cols in zip((r_own, r_oth), HALVES):
                u = dot(zv, rows_own_first(w.at[layer], order))
                ref[s : s + n, cols] = (ref[s : s + n, cols] + u).astype(BF).astype(F32)

    def block(k):
        a, b = A0 + 512 - 128 * k, PAD + 256 - 64 * k
        return ((xa, slice(a, a + 128)), (xp, slice(b, b + 64)))

    for layer, targets, far in ((7, (0, 2), 1), (8, (0,), 2)):
        t0, t1 = taps[layer, 0:1], taps[layer, 1:2]
        at = 0
        for k in targets:
            for (ref, now), (_, before) in zip(block(k), block(k + far)):
                n = now.stop - now.start
                y[at : at + n] = (t0 * ref[before] + t1 * ref[now]).astype(BF)
                at += n
        rows = at
        gated_units(y, z, rows, *gate(layer), order)
        z_out[layer] = z[0:192]
        zv = z[0:rows]
        for w, cols in zip((r_own, r_oth), HALVES):
            u = dot(zv, rows_own_first(w.at[layer], order))
            at = 0
            for k in targets:
                for ref, now in block(k):
                    n = now.stop - now.start
                    new = (ref[now, cols] + u[at : at + n]).astype(BF)
                    if layer == 8:
                        x_out[at : at + n, cols] = new
                    else:
                        ref[now, cols] = new.astype(F32)
                    at += n


def last_layer(x0, x4, taps, g_own, g_oth, r_own, r_oth, out, y):
    _, order = row_order()
    t0, t1 = taps[9, 0:1], taps[9, 1:2]
    y[...] = (t0 * x4[...].astype(F32) + t1 * x0[...].astype(F32)).astype(BF)
    z = out.at[192:384]
    gated_units(y, z, 192, (g_own, g_oth), 1024 * (9 - SPLIT), order)
    zv = z[...]
    for r, cols in zip((r_own, r_oth), HALVES):
        out[0:192, cols] = (x0[:, cols].astype(F32) + dot(zv, rows_own_first(r.at[9], order))).astype(BF)


def skip_kernel(z_own, z_oth, w, out):
    _, order = row_order()
    for z, at, rows in ((z_own, 0, order), (z_oth, 192, order[::-1])):
        total = dot(z[0], rows_own_first(w.at[0], rows))
        for layer in range(1, 9):
            total = total + dot(z[layer], rows_own_first(w.at[layer], rows))
        out[at : at + 192] = total


def outputs_kernel(g, skip, w, stream, skips, mixed):
    core = lax.axis_index("chan")
    for me in range(2):

        @pl.when(core == me)
        def _(me=me):
            weights = {k: rows_own_first(w.at[9], (256 * k, 256 - 256 * k)) for k in range(2)}

            def fill(out, pieces):
                for k, rows in enumerate(pieces):
                    out[k] = rows[0:128].astype(BF)
                    for j in range(2):
                        mixed[j, pl.ds(k, 64, stride=2)] = rows[128:192, 128 * j : 128 * j + 128]
                for j in range(2):
                    out[2, :, 128 * j : 128 * j + 128] = mixed[j].astype(BF)

            fill(stream, [g[k, 0:192, HALVES[0 if k == me else 1]].astype(F32) for k in range(2)])
            sums = (skip[0:192], skip[192:384])
            fill(skips, [sums[0 if k == me else 1] + dot(g[k, 192:384], weights[k]) for k in range(2)])


def call(body, inputs, outs, scratch, flops, spaces=None, vmem_mib=24):
    moved = sum(v.size * v.dtype.itemsize for v in inputs)
    vmem = pl.BlockSpec(memory_space=pltpu.VMEM)
    return pl.pallas_call(
        body,
        out_shape=outs,
        in_specs=[pl.BlockSpec(memory_space=one) for one in spaces or [pltpu.VMEM] * len(inputs)],
        out_specs=jax.tree.map(lambda _: vmem, outs),
        scratch_shapes=scratch,
        cost_estimate=pl.CostEstimate(flops=flops, bytes_accessed=moved, transcendentals=0),
        compiler_params=pltpu.CompilerParams(vmem_limit_bytes=vmem_mib * 2**20),
    )(*inputs)


def relayout_kernel(first, count, *refs):
    *taps, w, out, raw, sems = refs
    copies = [pltpu.make_async_copy(w.at[first + i], raw.at[i], sems.at[i]) for i in range(count)]
    for copy in copies:
        copy.start()
    for tap in range(2 if taps else 0):
        rest = taps[0][:, tap]
        for part in range(3):
            value = rest.astype(BF)
            rest = rest - value.astype(F32)
            at = count * 1024 + 48 * tap + 16 * part
            out[at : at + 10] = value
            out[at + 10 : at + 16] = jnp.zeros((6, 256), BF)
    for i, copy in enumerate(copies):
        copy.wait()
        both = raw[i].reshape(512, 512)
        out[1024 * i : 1024 * i + 512] = both[:, :256]
        out[1024 * i + 512 : 1024 * i + 1024] = both[:, 256:]


def relayout(first, count, vmem_mib, w_gate, *taps):
    return call(
        functools.partial(relayout_kernel, first, count),
        [*taps, w_gate],
        jax.ShapeDtypeStruct((count * 1024 + 96 * len(taps), 256), BF),
        [pltpu.VMEM((count, 512, 2, 256), BF), pltpu.SemaphoreType.DMA((count,))],
        10**6,
        [pltpu.VMEM] * len(taps) + [pltpu.HBM],
        vmem_mib,
    )


def local(signal, taps, w_gate, w_res, w_skip):
    sds = jax.ShapeDtypeStruct
    vm = pltpu.VMEM
    own = lax.all_gather(signal, "chan", axis=2, tiled=True)
    h1 = from_two(own, (1, 2))
    h2 = from_two(own, (4, 3))
    r_oth = other_core(w_res)
    ga_own = relayout(0, SPLIT, MIB_A, w_gate)
    ga_oth = other_core(ga_own)
    gb_own = relayout(SPLIT, 10 - SPLIT, MIB_B, w_gate, taps)
    gb_oth = other_core(gb_own)
    h1 = lax.all_gather(h1, "chan", axis=0)
    h2 = lax.all_gather(h2, "chan", axis=0)
    x9, zs, taps_all = call(
        first_kernel,
        [own, h1, h2, taps, ga_own, ga_oth, gb_own, gb_oth, w_res, r_oth],
        (sds((192, 512), BF), sds((9, 192, 512), BF), sds((10, 2, 512), F32)),
        [
            vm((PAD + 640, 512), F32),
            vm((4, PAD + 640, 128), F32),
            vm((PAD + 320, 512), F32),
            vm((960, 512), BF),
            vm((960, 512), BF),
        ],
        7000 * 512 * 1536 * 2,
    )
    x9_far = from_earlier(x9, 4)
    zs_oth = other_core(zs)
    skip = call(skip_kernel, [zs, zs_oth, w_skip], sds((384, 256), F32), [], 9 * 192 * 512 * 512 * 2)
    both = call(
        last_layer,
        [x9, x9_far, taps_all, gb_own, gb_oth, w_res, r_oth],
        sds((384, 512), BF),
        [vm((192, 512), BF)],
        192 * 512 * 1536 * 2,
    )
    both = lax.all_gather(both, "chan", axis=0)
    return call(
        outputs_kernel,
        [both, skip, w_skip],
        (sds((3, 128, 256), BF), sds((3, 128, 256), BF)),
        [vm((2, 128, 128), F32)],
        384 * 512 * 256 * 2,
    )


def solution(mesh):
    in_specs = (
        P(None, "tm", "chan"),
        P(None, None, "chan"),
        P(None, None, None, "chan"),
        P(None, None, "chan"),
        P(None, None, "chan"),
    )
    out_specs = (P(None, "tm", "chan"), P(None, "tm", "chan"))
    return jax.shard_map(local, mesh=mesh, in_specs=in_specs, out_specs=out_specs, check_vma=False)
```

```python
import functools

import jax
import jax.numpy as jnp
from jax import lax
from jax.experimental import pallas as pl
from jax.experimental.pallas import tpu as pltpu
from jax.sharding import PartitionSpec as P


PAD = 16
MIB_A, MIB_B = 47, 24
SPLIT = 5
A0 = PAD
A_FIRST = (0, 0, 0, 16, 32, 64, 128)
B_FIRST = (0, 0, 0, 0, 16, 32, 64)
HALVES = (slice(0, 256), slice(256, 512))
BF = jnp.bfloat16
F32 = jnp.float32


def from_earlier(value, steps):
    count = lax.axis_size("tm")
    return lax.ppermute(value, "tm", [(i, i + steps) for i in range(count - steps)])


def from_two(value, steps):
    count = lax.axis_size("tm")
    pairs = [(2 * i + c, 2 * (i + steps[c]) + c) for c in range(2) for i in range(count - steps[c])]
    return lax.ppermute(value, ("tm", "chan"), pairs)


def other_core(value):
    return lax.ppermute(value, "chan", [(0, 1), (1, 0)])


def dot(a, b):
    return jnp.dot(a, b, preferred_element_type=F32)


def row_order():
    core = lax.axis_index("chan")
    return core, (pl.multiple_of(core * 256, 256), pl.multiple_of(256 - core * 256, 256))


def rows_own_first(w, order, at=0):
    return jnp.concatenate([w[pl.ds(at + start, 256)] for start in order], axis=0)


def gated_units(y_ref, z_ref, rows, weights, at, order):
    y = y_ref[0:rows]
    for w, cols in zip(weights, HALVES):
        f = dot(y, rows_own_first(w, order, at))
        g = dot(y, rows_own_first(w, order, at + 512))
        z_ref[0:rows, cols] = (jnp.tanh(f) * (0.5 + 0.5 * jnp.tanh(0.5 * g))).astype(BF)


def first_kernel(own, h1, h2, t_own, ga_own, ga_oth, gb_own, gb_oth, r_own, r_oth, x_out, z_out, taps, xa, xb, xp, y, z):
    core, order = row_order()
    taps[:, :, HALVES[0]] = t_own[...]
    for tap in range(2):
        at = 1024 * (10 - SPLIT) + 48 * tap
        parts = [gb_oth[at + 16 * part : at + 16 * part + 10].astype(F32) for part in range(3)]
        taps[:, tap, HALVES[1]] = parts[0] + parts[1] + parts[2]

    def gate(layer):
        return ((ga_own, ga_oth), 1024 * layer) if layer < SPLIT else ((gb_own, gb_oth), 1024 * (layer - SPLIT))

    zero = jnp.zeros((PAD, 512), F32)
    xa[0:PAD] = zero
    xb[:, 0:PAD] = jnp.zeros((4, PAD, 128), F32)
    xp[0:PAD] = zero
    blocks = ((h2, 0), (h2, 1), (h1, 0), (h1, 1))

    def load(rows, source):
        for start, cols in zip(order, HALVES):
            given = pl.ds(start, 256)
            xa[rows, cols] = source[core, :, given].astype(F32)
            shared = source[2, :, given].astype(F32)
            for j in range(2):
                xb[cols.start // 128 + j, rows] = shared[:, 128 * j : 128 * j + 128]

    for k, (h, i) in enumerate(blocks):
        load(slice(A0 + 128 * k, A0 + 128 * k + 128), h.at[i])
    load(slice(A0 + 512, A0 + 640), own)

    for layer in range(7):
        delay = 2**layer
        first, first_b = A_FIRST[layer], B_FIRST[layer]
        na, nb = 640 - first, 320 - first_b
        rows = na + nb
        t0, t1 = taps[layer, 0:1], taps[layer, 1:2]
        s = A0 + first
        y[0:na] = (t0 * xa[s - delay : s - delay + na] + t1 * xa[s : s + na]).astype(BF)
        if layer == 0:
            for j in range(4):
                lanes = slice(128 * j, 128 * j + 128)
                now = xb[j, pl.ds(PAD + core, 320, stride=2)]
                before = xb[j, pl.ds(PAD - 1 + core, 320, stride=2)]
                y[640:960, lanes] = (t0[:, lanes] * before + t1[:, lanes] * now).astype(BF)
                xp[PAD : PAD + 320, lanes] = now
        else:
            s = PAD + first_b
            half = delay // 2
            y[na:rows] = (t0 * xp[s - half : s - half + nb] + t1 * xp[s : s + nb]).astype(BF)
        for lo, hi in ((0, na), (na, rows)):
            gated_units(y.at[lo:hi], z.at[lo:hi], hi - lo, *gate(layer), order)
        z_out[layer, 0:128] = z[na - 128 : na]
        z_out[layer, 128:192] = z[rows - 64 : rows]
        for ref, s, n, at in ((xa, A0 + first, na, 0), (xp, PAD + first_b, nb, na)):
            zv = z[at : at + n]
            for w, cols in zip((r_own, r_oth), HALVES):
                u = dot(zv, rows_own_first(w.at[layer], order))
                ref[s : s + n, cols] = (ref[s : s + n, cols] + u).astype(BF).astype(F32)

    def block(k):
        a, b = A0 + 512 - 128 * k, PAD + 256 - 64 * k
        return ((xa, slice(a, a + 128)), (xp, slice(b, b + 64)))

    for layer, targets, far in ((7, (0, 2), 1), (8, (0,), 2)):
        t0, t1 = taps[layer, 0:1], taps[layer, 1:2]
        at = 0
        for k in targets:
            for (ref, now), (_, before) in zip(block(k), block(k + far)):
                n = now.stop - now.start
                y[at : at + n] = (t0 * ref[before] + t1 * ref[now]).astype(BF)
                at += n
        rows = at
        gated_units(y, z, rows, *gate(layer), order)
        z_out[layer] = z[0:192]
        zv = z[0:rows]
        for w, cols in zip((r_own, r_oth), HALVES):
            u = dot(zv, rows_own_first(w.at[layer], order))
            at = 0
            for k in targets:
                for ref, now in block(k):
                    n = now.stop - now.start
                    new = (ref[now, cols] + u[at : at + n]).astype(BF)
                    if layer == 8:
                        x_out[at : at + n, cols] = new
                    else:
                        ref[now, cols] = new.astype(F32)
                    at += n


def last_layer(x0, x4, taps, g_own, g_oth, r_own, r_oth, out, y):
    _, order = row_order()
    t0, t1 = taps[9, 0:1], taps[9, 1:2]
    y[...] = (t0 * x4[...].astype(F32) + t1 * x0[...].astype(F32)).astype(BF)
    z = out.at[192:384]
    gated_units(y, z, 192, (g_own, g_oth), 1024 * (9 - SPLIT), order)
    zv = z[...]
    for r, cols in zip((r_own, r_oth), HALVES):
        out[0:192, cols] = (x0[:, cols].astype(F32) + dot(zv, rows_own_first(r.at[9], order))).astype(BF)


def skip_kernel(z_own, z_oth, w, out):
    _, order = row_order()
    for z, at, rows in ((z_own, 0, order), (z_oth, 192, order[::-1])):
        total = dot(z[0], rows_own_first(w.at[0], rows))
        for layer in range(1, 9):
            total = total + dot(z[layer], rows_own_first(w.at[layer], rows))
        out[at : at + 192] = total


def outputs_kernel(g, skip, w, stream, skips, mixed):
    core = lax.axis_index("chan")
    for me in range(2):

        @pl.when(core == me)
        def _(me=me):
            weights = {k: rows_own_first(w.at[9], (256 * k, 256 - 256 * k)) for k in range(2)}

            def fill(out, pieces):
                for k, rows in enumerate(pieces):
                    out[k] = rows[0:128].astype(BF)
                    for j in range(2):
                        mixed[j, pl.ds(k, 64, stride=2)] = rows[128:192, 128 * j : 128 * j + 128].astype(F32)
                for j in range(2):
                    out[2, :, 128 * j : 128 * j + 128] = mixed[j].astype(BF)

            fill(stream, [g[k, 0:192, HALVES[0 if k == me else 1]] for k in range(2)])
            sums = (skip[0:192], skip[192:384])
            fill(skips, [sums[0 if k == me else 1] + dot(g[k, 192:384], weights[k]) for k in range(2)])


def call(body, inputs, outs, scratch, flops, spaces=None, vmem_mib=24):
    moved = sum(v.size * v.dtype.itemsize for v in inputs)
    vmem = pl.BlockSpec(memory_space=pltpu.VMEM)
    return pl.pallas_call(
        body,
        out_shape=outs,
        in_specs=[pl.BlockSpec(memory_space=one) for one in spaces or [pltpu.VMEM] * len(inputs)],
        out_specs=jax.tree.map(lambda _: vmem, outs),
        scratch_shapes=scratch,
        cost_estimate=pl.CostEstimate(flops=flops, bytes_accessed=moved, transcendentals=0),
        compiler_params=pltpu.CompilerParams(vmem_limit_bytes=vmem_mib * 2**20),
    )(*inputs)


def relayout_kernel(first, count, *refs):
    *taps, w, out, raw, sems = refs
    copies = [pltpu.make_async_copy(w.at[first + i], raw.at[i], sems.at[i]) for i in range(count)]
    for copy in copies:
        copy.start()
    for tap in range(2 if taps else 0):
        rest = taps[0][:, tap]
        for part in range(3):
            value = rest.astype(BF)
            rest = rest - value.astype(F32)
            at = count * 1024 + 48 * tap + 16 * part
            out[at : at + 10] = value
            out[at + 10 : at + 16] = jnp.zeros((6, 256), BF)
    for i, copy in enumerate(copies):
        copy.wait()
        both = raw[i].reshape(512, 512)
        out[1024 * i : 1024 * i + 512] = both[:, :256]
        out[1024 * i + 512 : 1024 * i + 1024] = both[:, 256:]


def relayout(first, count, vmem_mib, w_gate, *taps):
    return call(
        functools.partial(relayout_kernel, first, count),
        [*taps, w_gate],
        jax.ShapeDtypeStruct((count * 1024 + 96 * len(taps), 256), BF),
        [pltpu.VMEM((count, 512, 2, 256), BF), pltpu.SemaphoreType.DMA((count,))],
        10**6,
        [pltpu.VMEM] * len(taps) + [pltpu.HBM],
        vmem_mib,
    )


def local(signal, taps, w_gate, w_res, w_skip):
    sds = jax.ShapeDtypeStruct
    vm = pltpu.VMEM
    own = lax.all_gather(signal, "chan", axis=2, tiled=True)
    h1 = from_two(own, (2, 1))
    h2 = from_two(own, (4, 3))
    r_oth = other_core(w_res)
    ga_own = relayout(0, SPLIT, MIB_A, w_gate)
    ga_oth = other_core(ga_own)
    gb_own = relayout(SPLIT, 10 - SPLIT, MIB_B, w_gate, taps)
    gb_oth = other_core(gb_own)
    h1 = lax.all_gather(h1, "chan", axis=0)
    h2 = lax.all_gather(h2, "chan", axis=0)
    x9, zs, taps_all = call(
        first_kernel,
        [own, h1, h2, taps, ga_own, ga_oth, gb_own, gb_oth, w_res, r_oth],
        (sds((192, 512), BF), sds((9, 192, 512), BF), sds((10, 2, 512), F32)),
        [
            vm((PAD + 640, 512), F32),
            vm((4, PAD + 640, 128), F32),
            vm((PAD + 320, 512), F32),
            vm((960, 512), BF),
            vm((960, 512), BF),
        ],
        7000 * 512 * 1536 * 2,
    )
    x9_far = from_earlier(x9, 4)
    zs_oth = other_core(zs)
    skip = call(skip_kernel, [zs, zs_oth, w_skip], sds((384, 256), F32), [], 9 * 192 * 512 * 512 * 2)
    both = call(
        last_layer,
        [x9, x9_far, taps_all, gb_own, gb_oth, w_res, r_oth],
        sds((384, 512), BF),
        [vm((192, 512), BF)],
        192 * 512 * 1536 * 2,
    )
    both = lax.all_gather(both, "chan", axis=0)
    return call(
        outputs_kernel,
        [both, skip, w_skip],
        (sds((3, 128, 256), BF), sds((3, 128, 256), BF)),
        [vm((2, 128, 128), F32)],
        384 * 512 * 256 * 2,
    )


def solution(mesh):
    in_specs = (
        P(None, "tm", "chan"),
        P(None, None, "chan"),
        P(None, None, None, "chan"),
        P(None, None, "chan"),
        P(None, None, "chan"),
    )
    out_specs = (P(None, "tm", "chan"), P(None, "tm", "chan"))
    return jax.shard_map(local, mesh=mesh, in_specs=in_specs, out_specs=out_specs, check_vma=False)
```
